32 devices in a mesh: feat: 8 (over z, x), samp: 4 (over y, core).
Axes of the slice: x: 2, y: 2, z: 4, core: 2. Of those that a mesh axis runs over, the one named last changes fastest.
Arguments:
- tiles: float32 [32, 64, 128, 128], P('feat', 'samp'), may hold values from -0.0625 to 0.0625
- row_index: int32 [32, 64], P('feat', 'samp'), may hold values from 0 to 511
- targets: float32 [2048, 128], P('samp'), may hold values from -15 to 15
- penalty: float32 [32, 128], P('feat'), may hold values from 0.8 to 8
- picks: int32 [3, 16], P(None, 'feat'), may hold values from 0 to 3, as said below
Outputs:
- weights: float32 [32, 128], P('feat')
- residual: float32 [2048, 128], P('samp')
- gaps: float32 [3], replicated
The draws below stay inside these ranges and needn't reach their ends.
Inputs may be any that keep to these rules, and one draw needn't show every extreme that they name: Within one iteration the 2 entries of one feature group, picks[t, g * 2 : (g + 1) * 2], are distinct local block numbers.
All inputs are finite; a program needn't handle non-finite values.
Results may differ from the reference program's by a relative error of at most 0.0003.
Values sent between devices are 32-bit elements; how exact they have to be, the bound alone decides.
A program may use at most 64 MiB of HBM per device.

```python
import jax
import jax.numpy as jnp
from jax import lax

FB_DEV = 4
RB = 512
K = 16
BATCH = 2
ITERS = 3
FBLOCKS = 32
SROWS = 2048
N_SAMP = 4


def draw_picks(key, part):
    groups = FBLOCKS // FB_DEV
    keyset = jax.random.split(key, ITERS * groups)
    orders = jax.vmap(lambda single: jax.random.permutation(single, FB_DEV)[:BATCH])(keyset)
    return orders.reshape(ITERS, groups * BATCH).astype(jnp.int32)


def draw_penalty(key, part):
    uniform_part = jax.random.uniform(jax.random.fold_in(key, 11), (FBLOCKS, 128), jnp.float32)
    position = 1.0 - jnp.arange(FBLOCKS, dtype=jnp.float32) / (FBLOCKS - 1)
    rising = 3.0
    factor = jnp.exp(uniform_part * jnp.log(2.0))
    return (factor * jnp.power(rising, position)[:, None]).astype(jnp.float32)


def draw_targets(key, part):
    position = jnp.arange(SROWS, dtype=jnp.float32) / (SROWS - 1)
    values = jax.random.truncated_normal(jax.random.fold_in(key, 29), -5.0, 5.0, (SROWS, 128), jnp.float32)
    rising = 3.0
    return (values * jnp.power(rising, position)[:, None]).astype(jnp.float32)


def place_ends(entries, own_key, low, top_value):
    spot = [jax.random.randint(jax.random.fold_in(own_key, axis), (), 0, length) for axis, length in enumerate(entries.shape)]
    widest = entries.shape.index(max(entries.shape))
    next_to = spot[:widest] + [(spot[widest] + 1) % entries.shape[widest]] + spot[widest + 1:]
    return entries.at[tuple(spot)].set(low).at[tuple(next_to)].set(top_value)


def block_scale(key, extent, shards, least, top_value):
    level = 1.0
    for dim, shards_of in shards:
        draws = jax.random.uniform(jax.random.fold_in(jax.random.fold_in(key, 6), dim), (shards_of,), jnp.float32, least / len(shards), top_value / len(shards))
        level = level * jnp.repeat(jnp.exp(draws), extent[dim] // shards_of).reshape((-1,) + (1,) * (len(extent) - 1 - dim))
    return level


def scatter_about(own_key, shape, scale, limit, cuts=(), held_as=jnp.bfloat16):
    gain = block_scale(own_key, shape, cuts, -0.22, 0.18) if cuts else 1.0
    result = jax.random.normal(own_key, shape, jnp.float32) * scale * gain
    return jnp.minimum(jnp.maximum(result, -limit), limit).astype(held_as)


def setup_inputs(seed: int = 0) -> dict:
    arg_keys = jax.random.split(jax.random.key(seed), 6)
    return {
        "tiles": scatter_about(arg_keys[0], (FBLOCKS, N_SAMP * K, 128, 128), (128 * K * N_SAMP) ** -0.5, 0.0625, ((0, 8), (1, 4)), jnp.float32),
        "row_index": place_ends(jax.random.randint(arg_keys[1], (FBLOCKS, N_SAMP * K), 0, RB), jax.random.fold_in(arg_keys[1], 1), 0, RB - 1).astype(jnp.int32),
        "targets": draw_targets(jax.random.fold_in(arg_keys[5], 71), 0),
        "penalty": draw_penalty(jax.random.fold_in(arg_keys[5], 71), 0),
        "picks": draw_picks(jax.random.fold_in(arg_keys[5], 71), 0),
    }


STEP_SCALE = 2.0
EPSILON = 1e-6


def reference(tiles, row_index, targets, penalty, picks):
    precise = lax.Precision.HIGHEST
    groups = FBLOCKS // FB_DEV
    offsets = (jnp.arange(N_SAMP * K, dtype=jnp.int32) // K) * RB
    global_rows = (row_index + offsets[None, :]).astype(jnp.int32)
    col_sq = jnp.sum(tiles * tiles, axis=(1, 2))
    residual = -targets
    weights = jnp.zeros((FBLOCKS, 128), jnp.float32)
    base = None
    gap_list = []
    for iteration in range(ITERS):
        fetched = residual[global_rows]
        grad = jnp.einsum('bjrf,bjr->bf', tiles, fetched, precision=precise)
        sum_rr = jnp.sum(residual * residual)
        sum_ry = jnp.sum(residual * targets)
        if iteration == 0:
            base = sum_rr
        scale = jnp.min(penalty / jnp.maximum(jnp.abs(grad), penalty))
        norm_one = jnp.sum(penalty * jnp.abs(weights))
        gap_value = (0.5 * sum_rr + norm_one + 0.5 * scale * scale * sum_rr + scale * sum_ry) / (0.5 * base)
        gap_list.append(gap_value)
        chosen = (picks[iteration].reshape(groups, BATCH) + (jnp.arange(groups, dtype=jnp.int32) * FB_DEV)[:, None]).reshape(-1)
        marker = jnp.zeros((FBLOCKS,), jnp.float32).at[chosen].set(1.0)
        denom = STEP_SCALE * (col_sq + EPSILON)
        moved = weights - grad / denom
        shrunk = jnp.sign(moved) * jnp.maximum(jnp.abs(moved) - penalty / denom, 0.0)
        delta = (shrunk - weights) * marker[:, None]
        weights = weights + delta
        contrib = jnp.einsum('bjrf,bf->bjr', tiles, delta, precision=precise)
        residual = residual + jax.ops.segment_sum(contrib.reshape(-1, 128), global_rows.reshape(-1), num_segments=SROWS)
    return weights, residual, jnp.stack(gap_list)
```

```python
import functools

import jax
import jax.numpy as jnp
from jax import lax
from jax.experimental import pallas as pl
from jax.experimental.pallas import tpu as pltpu
from jax.sharding import PartitionSpec as P

STEP_SCALE = 2.0
EPSILON = 1e-06
MESH = pl.DeviceIdType.MESH
UNROLL_PEERS = 8


def each(count, body):
    if count <= UNROLL_PEERS:
        for d in range(1, count):
            body(d)
    else:
        lax.fori_loop(1, count, lambda d, c: (body(d), c)[1], 0)


def split3(v):
    hi = v.astype(jnp.bfloat16)
    rest = v - hi.astype(jnp.float32)
    mid = rest.astype(jnp.bfloat16)
    low = (rest - mid.astype(jnp.float32)).astype(jnp.bfloat16)
    return jnp.concatenate([hi, mid, low], axis=1)


def join3(p):
    w = p.shape[1] // 3
    return p[:, :w] + (p[:, w : 2 * w] + p[:, 2 * w :])


def kernel(
    nf, ns, tiles_hbm, rows_s, targets, penalty, picks,
    weights, residual, gaps,
    tiles_v, tiles_t, fetched, own_rows, rows_all, gbuf, vbuf, stat_f, stat_s,
    delta_buf, colsq, parts, hot_f, hot_r,
    dma_sem, fsend, frecv, ssend, srecv,
):
    iters, batch = picks.shape
    fb, k_tiles = rows_s.shape
    w = tiles_hbm.shape[-1]
    lanes = rows_all.shape[2]
    per = batch * k_tiles
    f_me, s_me = lax.axis_index("feat"), lax.axis_index("samp")
    half = k_tiles // 2

    def tile_copy(b, h):
        return pltpu.make_async_copy(
            tiles_hbm.at[b, pl.ds(h * half, half)],
            tiles_v.at[b, pl.ds(h * half, half)],
            dma_sem.at[b, h],
        )

    for b in range(fb):
        for h in range(2):
            tile_copy(b, h).start()

    barrier = pltpu.get_barrier_semaphore()
    each(nf, lambda d: pl.semaphore_signal(
        barrier, inc=1, device_id={"feat": lax.rem(f_me + d, nf)}, device_id_type=MESH))
    each(ns, lambda d: pl.semaphore_signal(
        barrier, inc=1, device_id={"samp": lax.rem(s_me + d, ns)}, device_id_type=MESH))

    def feat_copy(r, ref, d, slot):
        return pltpu.make_async_remote_copy(
            src_ref=ref.at[slot], dst_ref=ref.at[slot],
            send_sem=fsend.at[r, d], recv_sem=frecv.at[r, slot],
            device_id={"feat": lax.rem(f_me + d, nf)}, device_id_type=MESH)

    def samp_copy(r, ref, d, slot):
        return pltpu.make_async_remote_copy(
            src_ref=ref.at[slot], dst_ref=ref.at[slot],
            send_sem=ssend.at[r, d], recv_sem=srecv.at[r, slot],
            device_id={"samp": lax.rem(s_me + d, ns)}, device_id_type=MESH)

    def feat_send(r, ref):
        each(nf, lambda d: feat_copy(r, ref, d, f_me).start())

    def feat_wait(r, ref):
        each(nf, lambda d: feat_copy(r, ref, d, lax.rem(f_me + d, nf)).wait_recv())

    def samp_send(r, ref):
        each(ns, lambda d: samp_copy(r, ref, d, s_me).start())

    def samp_wait(r, ref):
        each(ns, lambda d: samp_copy(r, ref, d, lax.rem(s_me + d, ns)).wait_recv())

    lane = lax.broadcasted_iota(jnp.int32, (1, lanes), 1)
    for t in range(iters):
        message = jnp.zeros((1, lanes), jnp.int32)
        for i in range(batch):
            p = picks[t, i]
            for k in range(k_tiles):
                message = jnp.where(lane == f_me * per + (i * k_tiles + k), rows_s[p, k], message)
        rows_all[f_me, pl.ds(t, 1), :] = message

    for b in range(fb):
        for k in range(k_tiles):
            row = rows_s[b, k]
            fetched[pl.ds(b * k_tiles + k, 1), :] = -targets[pl.ds(row, 1), :]
            own_rows[pl.ds(b * k_tiles + k, 1), :] = jnp.full((1, w), row, jnp.int32)

    pl.semaphore_wait(barrier, (nf - 1) + (ns - 1))
    feat_send(0, rows_all)

    target = targets[...]
    residual[...] = -target
    square = jnp.sum(target * target, axis=0, keepdims=True)
    stat_s[s_me, pl.ds(0, 1), :] = square
    stat_s[s_me, pl.ds(iters, 1), :] = -square

    g0 = gbuf.at[0]

    def first(b, carry):
        acc = jnp.zeros((w, w), jnp.float32)
        sq = jnp.zeros((8, w), jnp.float32)
        for h in range(2):
            tile_copy(b, h).wait()
            for k in range(h * half, (h + 1) * half):
                tile = tiles_v[b, k]
                turned = tile.T
                tiles_t[b, k] = turned
                acc = acc + turned * fetched[pl.ds(b * k_tiles + k, 1), :]
                sq = sq + jnp.sum((tile * tile).reshape(w // 8, 8, w), axis=0)
        g0[s_me, pl.ds(b, 1), :] = jnp.sum(acc.T, axis=0, keepdims=True)
        g0[s_me, pl.ds(fb + b, 1), :] = jnp.sum(sq, axis=0, keepdims=True)
        return carry

    lax.fori_loop(0, fb, first, 0)
    weights[...] = jnp.zeros_like(weights)

    for t in range(iters):
        gt = gbuf.at[t]
        if t > 0:
            def later(b, carry, gt=gt):
                acc = jnp.zeros((w, w), jnp.float32)
                for k in range(k_tiles):
                    acc = acc + tiles_t[b, k] * fetched[pl.ds(b * k_tiles + k, 1), :]
                gt[s_me, pl.ds(b, 1), :] = jnp.sum(acc.T, axis=0, keepdims=True)
                return carry

            lax.fori_loop(0, fb, later, 0)
        samp_send(t, gt)
        if t > 0:
            residual[...] += join3(jnp.dot(
                hot_r[...], parts[...], preferred_element_type=jnp.float32))
            res = residual[...]
            stat_s[s_me, pl.ds(t, 1), :] = jnp.sum(res * res, axis=0, keepdims=True)
            stat_s[s_me, pl.ds(iters + t, 1), :] = jnp.sum(
                res * targets[...], axis=0, keepdims=True)
        else:
            feat_wait(0, rows_all)
        if t == iters - 1:
            samp_send(iters, stat_s)
        samp_wait(t, gt)
        total = gt[0]
        for s in range(1, ns):
            total = total + gt[s]
        grad = total[:fb]
        if t == 0:
            colsq[...] = total[fb:]
        pen = penalty[...]
        old = weights[...]
        denom = STEP_SCALE * (colsq[...] + EPSILON)
        moved = old - grad / denom
        size = jnp.maximum(jnp.abs(moved) - pen / denom, 0.0)
        block = lax.broadcasted_iota(jnp.int32, (fb, w), 0)
        picked = block == picks[t, 0]
        for i in range(1, batch):
            picked = picked | (block == picks[t, i])
        delta = jnp.where(picked, jnp.where(moved >= 0.0, size, -size) - old, 0.0)
        delta_buf[...] = delta
        vt = vbuf.at[t]
        for i in range(batch):
            p = picks[t, i]
            column = jnp.broadcast_to(delta_buf[pl.ds(p, 1), :], (w, w)).T
            for k in range(k_tiles):
                vt[f_me, pl.ds(i * k_tiles + k, 1), :] = jnp.sum(
                    tiles_t[p, k] * column, axis=0, keepdims=True)
        feat_send(1 + t, vt)
        stat_f[f_me, pl.ds(t, 1), :] = jnp.min(
            pen / jnp.maximum(jnp.abs(grad), pen), axis=0, keepdims=True)
        stat_f[f_me, pl.ds(iters + t, 1), :] = jnp.sum(
            pen * jnp.abs(old), axis=0, keepdims=True)
        weights[...] = old + delta
        if t == iters - 1:
            feat_send(1 + iters, stat_f)
        rows_t = rows_all[0, pl.ds(t, 1), :]
        for f in range(1, nf):
            rows_t = rows_t + rows_all[f, pl.ds(t, 1), :]
        if t < iters - 1:
            own = jnp.concatenate([own_rows[...]] * (lanes // w), axis=1)
            hot_f[...] = jnp.where(own == rows_t, 1.0, 0.0).astype(jnp.bfloat16)
        number = lax.broadcasted_iota(jnp.int32, hot_r.shape, 0)
        hot_r[...] = jnp.where(number == rows_t, 1.0, 0.0).astype(jnp.bfloat16)
        feat_wait(1 + t, vt)
        split = split3(vt[...].reshape(lanes, w))
        if t < iters - 1:
            parts[...] = split
            fetched[...] += join3(jnp.dot(
                hot_f[...], split, preferred_element_type=jnp.float32))
        else:
            residual[...] += join3(jnp.dot(
                hot_r[...], split, preferred_element_type=jnp.float32))

    samp_wait(iters, stat_s)
    feat_wait(1 + iters, stat_f)
    stats = stat_s[0]
    for s in range(1, ns):
        stats = stats + stat_s[s]
    low, norm = stat_f[0], stat_f[0]
    for f in range(1, nf):
        low, norm = jnp.minimum(low, stat_f[f]), norm + stat_f[f]
    rr = jnp.sum(stats[:iters], axis=1, keepdims=True)
    ry = jnp.sum(stats[iters : 2 * iters], axis=1, keepdims=True)
    scale = jnp.min(low[:iters], axis=1, keepdims=True)
    norm_one = jnp.sum(norm[iters : 2 * iters], axis=1, keepdims=True)
    value = (0.5 * rr + norm_one + 0.5 * scale * scale * rr + scale * ry) / (0.5 * rr[0:1])
    for t in range(iters):
        gaps[t] = jnp.sum(value[t : t + 1])

    def drain_feat(d):
        feat_copy(0, rows_all, d, f_me).wait_send()
        for t in range(iters):
            feat_copy(1 + t, vbuf.at[t], d, f_me).wait_send()
        feat_copy(1 + iters, stat_f, d, f_me).wait_send()

    def drain_samp(d):
        for t in range(iters):
            samp_copy(t, gbuf.at[t], d, s_me).wait_send()
        samp_copy(iters, stat_s, d, s_me).wait_send()

    each(nf, drain_feat)
    each(ns, drain_samp)


def solution(mesh):
    nf, ns = mesh.shape["feat"], mesh.shape["samp"]

    def shards(tiles, row_index, targets, penalty, picks):
        fb, k_tiles, w, _ = tiles.shape
        iters, batch = picks.shape
        rb = targets.shape[0]
        per = batch * k_tiles
        lanes = nf * per
        stat_rows = -(-2 * iters // 8) * 8
        vmem, smem = pltpu.VMEM, pltpu.SMEM
        f32, i32 = jnp.float32, jnp.int32
        spec = lambda space: pl.BlockSpec(memory_space=space)
        return pl.pallas_call(
            functools.partial(kernel, nf, ns),
            out_shape=(
                jax.ShapeDtypeStruct((fb, w), f32),
                jax.ShapeDtypeStruct((rb, w), f32),
                jax.ShapeDtypeStruct((iters,), f32),
            ),
            in_specs=[spec(pl.ANY), spec(smem), spec(vmem), spec(vmem), spec(smem)],
            out_specs=(spec(vmem), spec(vmem), spec(smem)),
            scratch_shapes=[
                vmem((fb, k_tiles, w, w), f32),
                vmem((fb, k_tiles, w, w), f32),
                vmem((fb * k_tiles, w), f32),
                vmem((fb * k_tiles, w), i32),
                vmem((nf, -(-iters // 8) * 8, lanes), i32),
                vmem((iters, ns, 2 * fb, w), f32),
                vmem((iters, nf, per, w), f32),
                vmem((nf, stat_rows, w), f32),
                vmem((ns, stat_rows, w), f32),
                vmem((fb, w), f32),
                vmem((fb, w), f32),
                vmem((lanes, 3 * w), jnp.bfloat16),
                vmem((fb * k_tiles, lanes), jnp.bfloat16),
                vmem((rb, lanes), jnp.bfloat16),
                pltpu.SemaphoreType.DMA((fb, 2)),
                pltpu.SemaphoreType.DMA((iters + 2, nf)),
                pltpu.SemaphoreType.DMA((iters + 2, nf)),
                pltpu.SemaphoreType.DMA((iters + 1, ns)),
                pltpu.SemaphoreType.DMA((iters + 1, ns)),
            ],
            compiler_params=pltpu.CompilerParams(collective_id=0, has_side_effects=True),
        )(tiles, row_index, targets, penalty, picks)

    return jax.shard_map(
        shards,
        mesh=mesh,
        in_specs=(
            P("feat", "samp", None, None),
            P("feat", "samp"),
            P("samp", None),
            P("feat", None),
            P(None, "feat"),
        ),
        out_specs=(P("feat", None), P("samp", None), P()),
        check_vma=False,
    )
```

```python
import functools

import jax
import jax.numpy as jnp
from jax import lax
from jax.experimental import pallas as pl
from jax.experimental.pallas import tpu as pltpu
from jax.sharding import PartitionSpec as P

STEP_SCALE = 2.0
EPSILON = 1e-06
MESH = pl.DeviceIdType.MESH
UNROLL_PEERS = 8


def each(count, body):
    if count <= UNROLL_PEERS:
        for d in range(count - 1, 0, -1):
            body(d)
    else:
        lax.fori_loop(1, count, lambda d, c: (body(d), c)[1], 0)


def partner(me, d, count):
    if not isinstance(d, int) or count & (count - 1):
        return lax.rem(me + d, count)
    other, bit = 0, 1
    while bit < count:
        v = lax.rem(lax.div(me, bit), 2)
        other = other + bit * (1 - v if d & bit else v)
        bit *= 2
    return other


def split3(v):
    hi = v.astype(jnp.bfloat16)
    rest = v - hi.astype(jnp.float32)
    mid = rest.astype(jnp.bfloat16)
    low = (rest - mid.astype(jnp.float32)).astype(jnp.bfloat16)
    return jnp.concatenate([hi, mid, low], axis=1)


def join3(p):
    w = p.shape[1] // 3
    return p[:, :w] + (p[:, w : 2 * w] + p[:, 2 * w :])


def kernel(
    nf, ns, tiles_hbm, rows_hbm, targets_hbm, penalty_hbm, picks_hbm,
    weights, residual, gaps,
    rows_s, picks, targets, penalty, tiles_v, tiles_t, fetched, own_rows, rows_all, gbuf, vbuf, stat_f, stat_s,
    delta_buf, colsq, parts, hot_f, hot_r,
    in_sem, dma_sem, fsend, frecv, ssend, srecv,
):
    batch, iters = picks.shape
    fb, k_tiles = rows_s.shape
    w = tiles_hbm.shape[-1]
    lanes = rows_all.shape[2]
    per = batch * k_tiles
    f_me, s_me = lax.axis_index("feat"), lax.axis_index("samp")
    half = k_tiles // 2

    def tile_copy(b, h):
        return pltpu.make_async_copy(
            tiles_hbm.at[b, pl.ds(h * half, half)],
            tiles_v.at[b, pl.ds(h * half, half)],
            dma_sem.at[b, h],
        )

    small = [
        pltpu.make_async_copy(src, dst, in_sem.at[n])
        for n, (src, dst) in enumerate((
            (rows_hbm, rows_s), (picks_hbm, picks), (targets_hbm, targets), (penalty_hbm, penalty)))
    ]
    for copy in small:
        copy.start()
    for b in range(fb):
        for h in range(2):
            tile_copy(b, h).start()

    barrier = pltpu.get_barrier_semaphore()
    each(nf, lambda d: pl.semaphore_signal(
        barrier, inc=1, device_id={"feat": partner(f_me, d, nf)}, device_id_type=MESH))
    each(ns, lambda d: pl.semaphore_signal(
        barrier, inc=1, device_id={"samp": partner(s_me, d, ns)}, device_id_type=MESH))

    def feat_copy(r, ref, d, slot):
        return pltpu.make_async_remote_copy(
            src_ref=ref.at[slot], dst_ref=ref.at[slot],
            send_sem=fsend.at[r, d], recv_sem=frecv.at[r, slot],
            device_id={"feat": partner(f_me, d, nf)}, device_id_type=MESH)

    def samp_copy(r, ref, d, slot):
        return pltpu.make_async_remote_copy(
            src_ref=ref.at[slot], dst_ref=ref.at[slot],
            send_sem=ssend.at[r, d], recv_sem=srecv.at[r, slot],
            device_id={"samp": partner(s_me, d, ns)}, device_id_type=MESH)

    def feat_send(r, ref):
        each(nf, lambda d: feat_copy(r, ref, d, f_me).start())

    def feat_wait(r, ref):
        each(nf, lambda d: feat_copy(r, ref, d, partner(f_me, d, nf)).wait_recv())

    def samp_send(r, ref):
        each(ns, lambda d: samp_copy(r, ref, d, s_me).start())

    def samp_wait(r, ref):
        each(ns, lambda d: samp_copy(r, ref, d, partner(s_me, d, ns)).wait_recv())

    small[0].wait()
    small[1].wait()

    lane = lax.broadcasted_iota(jnp.int32, (1, lanes), 1)
    for t in range(iters):
        message = jnp.zeros((1, lanes), jnp.int32)
        for i in range(batch):
            p = picks[i, t]
            for k in range(k_tiles):
                message = jnp.where(lane == f_me * per + (i * k_tiles + k), rows_s[p, k], message)
        rows_all[f_me, pl.ds(t, 1), :] = message

    small[2].wait()
    small[3].wait()
    for b in range(fb):
        for k in range(k_tiles):
            row = rows_s[b, k]
            fetched[pl.ds(b * k_tiles + k, 1), :] = -targets[pl.ds(row, 1), :]
            own_rows[pl.ds(b * k_tiles + k, 1), :] = jnp.full((1, w), row, jnp.int32)

    target = targets[...]
    residual[...] = -target
    square = jnp.sum(target * target, axis=0, keepdims=True)
    stat_s[s_me, pl.ds(0, 1), :] = square
    stat_s[s_me, pl.ds(iters, 1), :] = -square

    g0 = gbuf.at[0]

    def first(b, carry):
        acc = jnp.zeros((w, w), jnp.float32)
        sq = jnp.zeros((8, w), jnp.float32)
        for h in range(2):
            tile_copy(b, h).wait()
            for k in range(h * half, (h + 1) * half):
                tile = tiles_v[b, k]
                turned = tile.T
                tiles_t[b, k] = turned
                acc = acc + turned * fetched[pl.ds(b * k_tiles + k, 1), :]
                sq = sq + jnp.sum((tile * tile).reshape(w // 8, 8, w), axis=0)
        g0[s_me, pl.ds(b, 1), :] = jnp.sum(acc.T, axis=0, keepdims=True)
        g0[s_me, pl.ds(fb + b, 1), :] = jnp.sum(sq, axis=0, keepdims=True)
        return carry

    lax.fori_loop(0, fb, first, 0)
    weights[...] = jnp.zeros_like(weights)

    for t in range(iters):
        gt = gbuf.at[t]
        if t > 0:
            def later(b, carry, gt=gt):
                acc = jnp.zeros((w, w), jnp.float32)
                for k in range(k_tiles):
                    acc = acc + tiles_t[b, k] * fetched[pl.ds(b * k_tiles + k, 1), :]
                gt[s_me, pl.ds(b, 1), :] = jnp.sum(acc.T, axis=0, keepdims=True)
                return carry

            lax.fori_loop(0, fb, later, 0)
        if t == 0:
            pl.semaphore_wait(barrier, (nf - 1) + (ns - 1))
        samp_send(t, gt)
        if t == 0:
            feat_send(0, rows_all)
        if t > 0:
            residual[...] += join3(jnp.dot(
                hot_r[...], parts[...], preferred_element_type=jnp.float32))
            res = residual[...]
            stat_s[s_me, pl.ds(t, 1), :] = jnp.sum(res * res, axis=0, keepdims=True)
            stat_s[s_me, pl.ds(iters + t, 1), :] = jnp.sum(
                res * targets[...], axis=0, keepdims=True)
        if t == iters - 1:
            samp_send(iters, stat_s)
        samp_wait(t, gt)
        total = gt[0]
        for s in range(1, ns):
            total = total + gt[s]
        grad = total[:fb]
        if t == 0:
            colsq[...] = total[fb:]
        pen = penalty[...]
        old = weights[...]
        denom = STEP_SCALE * (colsq[...] + EPSILON)
        moved = old - grad / denom
        size = jnp.maximum(jnp.abs(moved) - pen / denom, 0.0)
        block = lax.broadcasted_iota(jnp.int32, (fb, w), 0)
        picked = block == picks[0, t]
        for i in range(1, batch):
            picked = picked | (block == picks[i, t])
        delta = jnp.where(picked, jnp.where(moved >= 0.0, size, -size) - old, 0.0)
        delta_buf[...] = delta
        vt = vbuf.at[t]
        for i in range(batch):
            p = picks[i, t]
            column = jnp.broadcast_to(delta_buf[pl.ds(p, 1), :], (w, w)).T
            for k in range(k_tiles):
                vt[f_me, pl.ds(i * k_tiles + k, 1), :] = jnp.sum(
                    tiles_t[p, k] * column, axis=0, keepdims=True)
        feat_send(1 + t, vt)
        stat_f[f_me, pl.ds(t, 1), :] = jnp.min(
            pen / jnp.maximum(jnp.abs(grad), pen), axis=0, keepdims=True)
        stat_f[f_me, pl.ds(iters + t, 1), :] = jnp.sum(
            pen * jnp.abs(old), axis=0, keepdims=True)
        weights[...] = old + delta
        if t == iters - 1:
            feat_send(1 + iters, stat_f)
        if t == 0:
            feat_wait(0, rows_all)
        rows_t = rows_all[0, pl.ds(t, 1), :]
        for f in range(1, nf):
            rows_t = rows_t + rows_all[f, pl.ds(t, 1), :]
        if t < iters - 1:
            own = jnp.concatenate([own_rows[...]] * (lanes // w), axis=1)
            hot_f[...] = jnp.where(own == rows_t, 1.0, 0.0).astype(jnp.bfloat16)
        number = lax.broadcasted_iota(jnp.int32, hot_r.shape, 0)
        hot_r[...] = jnp.where(number == rows_t, 1.0, 0.0).astype(jnp.bfloat16)
        feat_wait(1 + t, vt)
        split = split3(vt[...].reshape(lanes, w))
        if t < iters - 1:
            parts[...] = split
            fetched[...] += join3(jnp.dot(
                hot_f[...], split, preferred_element_type=jnp.float32))
        else:
            residual[...] += join3(jnp.dot(
                hot_r[...], split, preferred_element_type=jnp.float32))

    samp_wait(iters, stat_s)
    feat_wait(1 + iters, stat_f)
    stats = stat_s[0]
    for s in range(1, ns):
        stats = stats + stat_s[s]
    low, norm = stat_f[0], stat_f[0]
    for f in range(1, nf):
        low, norm = jnp.minimum(low, stat_f[f]), norm + stat_f[f]
    rr = jnp.sum(stats[:iters], axis=1, keepdims=True)
    ry = jnp.sum(stats[iters : 2 * iters], axis=1, keepdims=True)
    scale = jnp.min(low[:iters], axis=1, keepdims=True)
    norm_one = jnp.sum(norm[iters : 2 * iters], axis=1, keepdims=True)
    value = (0.5 * rr + norm_one + 0.5 * scale * scale * rr + scale * ry) / (0.5 * rr[0:1])
    gaps[...] = jnp.broadcast_to(value, gaps.shape)

    def drain_feat(d):
        feat_copy(0, rows_all, d, f_me).wait_send()
        for t in range(iters):
            feat_copy(1 + t, vbuf.at[t], d, f_me).wait_send()
        feat_copy(1 + iters, stat_f, d, f_me).wait_send()

    def drain_samp(d):
        for t in range(iters):
            samp_copy(t, gbuf.at[t], d, s_me).wait_send()
        samp_copy(iters, stat_s, d, s_me).wait_send()

    each(nf, drain_feat)
    each(ns, drain_samp)


def hand_out(weights_v, residual_v, gaps_v, weights, residual, gaps, sems):
    copies = [
        pltpu.make_async_copy(residual_v, residual, sems.at[0]),
        pltpu.make_async_copy(weights_v, weights, sems.at[1]),
    ]
    for copy in copies:
        copy.start()
    for t in range(gaps.shape[0]):
        gaps[t] = jnp.max(gaps_v[t : t + 1, :])
    for copy in copies:
        copy.wait()


def solution(mesh):
    nf, ns = mesh.shape["feat"], mesh.shape["samp"]

    def shards(tiles, row_index, targets, penalty, picks):
        fb, k_tiles, w, _ = tiles.shape
        picks = picks.T
        batch, iters = picks.shape
        rb = targets.shape[0]
        per = batch * k_tiles
        lanes = nf * per
        stat_rows = -(-2 * iters // 8) * 8
        vmem, smem = pltpu.VMEM, pltpu.SMEM
        f32, i32 = jnp.float32, jnp.int32
        spec = lambda space: pl.BlockSpec(memory_space=space)
        done = pl.pallas_call(
            functools.partial(kernel, nf, ns),
            out_shape=(vmem((fb, w), f32), vmem((rb, w), f32), vmem((iters, w), f32)),
            in_specs=[spec(pltpu.HBM)] * 5,
            out_specs=(spec(vmem),) * 3,
            scratch_shapes=[
                smem((fb, k_tiles), i32),
                smem((batch, iters), i32),
                vmem((rb, w), f32),
                vmem((fb, w), f32),
                vmem((fb, k_tiles, w, w), f32),
                vmem((fb, k_tiles, w, w), f32),
                vmem((fb * k_tiles, w), f32),
                vmem((fb * k_tiles, w), i32),
                vmem((nf, -(-iters // 8) * 8, lanes), i32),
                vmem((iters, ns, 2 * fb, w), f32),
                vmem((iters, nf, per, w), f32),
                vmem((nf, stat_rows, w), f32),
                vmem((ns, stat_rows, w), f32),
                vmem((fb, w), f32),
                vmem((fb, w), f32),
                vmem((lanes, 3 * w), jnp.bfloat16),
                vmem((fb * k_tiles, lanes), jnp.bfloat16),
                vmem((rb, lanes), jnp.bfloat16),
                pltpu.SemaphoreType.DMA((4,)),
                pltpu.SemaphoreType.DMA((fb, 2)),
                pltpu.SemaphoreType.DMA((iters + 2, nf)),
                pltpu.SemaphoreType.DMA((iters + 2, nf)),
                pltpu.SemaphoreType.DMA((iters + 1, ns)),
                pltpu.SemaphoreType.DMA((iters + 1, ns)),
            ],
            compiler_params=pltpu.CompilerParams(
                collective_id=0, has_side_effects=True, vmem_limit_bytes=24 * 1024 * 1024),
        )(*(pltpu.with_memory_space_constraint(a, pltpu.HBM)
            for a in (tiles, row_index, targets, penalty, picks)))
        return pl.pallas_call(
            hand_out,
            out_shape=(
                jax.ShapeDtypeStruct((fb, w), f32),
                jax.ShapeDtypeStruct((rb, w), f32),
                jax.ShapeDtypeStruct((iters,), f32),
            ),
            in_specs=[spec(vmem)] * 3,
            out_specs=(spec(pltpu.HBM), spec(pltpu.HBM), spec(smem)),
            scratch_shapes=[pltpu.SemaphoreType.DMA((2,))],
            compiler_params=pltpu.CompilerParams(vmem_limit_bytes=4 * 1024 * 1024),
        )(*(pltpu.with_memory_space_constraint(a, pltpu.VMEM) for a in done))

    return jax.shard_map(
        shards,
        mesh=mesh,
        in_specs=(
            P("feat", "samp", None, None),
            P("feat", "samp"),
            P("samp", None),
            P("feat", None),
            P(None, "feat"),
        ),
        out_specs=(P("feat", None), P("samp", None), P()),
        check_vma=False,
    )
```
